64 devices in a mesh: rep: 4 (over x, y), dp: 16 (over z, core).
Axes of the slice: x: 2, y: 2, z: 8, core: 2. Of those that a mesh axis runs over, the one named last changes fastest.
The devices are a block of a 4x4x8 slice.
Arguments:
- a: bfloat16 [64, 4, 4096, 896], P(('rep', 'dp')), parts along dimension 0
- g: bfloat16 [64, 4, 4096, 2560], P(('rep', 'dp')), parts along dimension 0
Outputs:
- output: bfloat16 [16, 896, 2560], P('rep'), parts along dimension 0
There are 4 independent parts. The reference program is written for one: setup_inputs(seed, part) draws one part's arguments, and reference() takes and returns one part's arrays. A program takes and returns all parts, laid end to end along the dimension named above; each array names one.
All inputs are finite; a program needn't handle non-finite values.
Results may differ from the reference program's by a relative error of at most 0.012.
Values are sent between devices in bfloat16 or wider.
A program may use at most 768 MiB of HBM per device.

```python
import jax
import jax.numpy as jnp
from jax import lax

DEVICES = 16
MATRICES = 4
TOKENS = 4096
D = 896
FF = 2560


def setup_inputs(seed: int = 0, part: int = 0) -> dict:
    ka, kg, ks = (jax.random.fold_in(k, part) for k in jax.random.split(jax.random.key(seed), 3))
    size = 2.0 ** jax.random.uniform(ks, (DEVICES, MATRICES, 1, 1), jnp.float32, -1.0, 1.0)
    a = jax.random.normal(ka, (DEVICES, MATRICES, TOKENS, D), jnp.float32)
    g = size * jax.random.normal(kg, (DEVICES, MATRICES, TOKENS, FF), jnp.float32) * (DEVICES * TOKENS) ** -0.5
    return {"a": a.astype(jnp.bfloat16), "g": g.astype(jnp.bfloat16)}


def reference(a, g):
    def take(so_far, one):
        return so_far + jnp.einsum("ntd,ntf->ndf", *one, preferred_element_type=jnp.float32), None

    return lax.scan(take, jnp.zeros((MATRICES, D, FF), jnp.float32), (a, g))[0].astype(jnp.bfloat16)
```

```python
import functools

import jax
import jax.numpy as jnp
from jax import lax
from jax.experimental import pallas as pl
from jax.experimental.pallas import tpu as pltpu
from jax.sharding import PartitionSpec as P

MESH = pl.DeviceIdType.MESH
CORES = 2
NB = 256
AB = 128
GSLOTS = 4
ROWS = 512


def kernel(devices, a_ref, g_ref, out_ref, at, gbuf, abuf, acc, stage, sums, gsem, asem, stage_sem, sums_sem,
           ring_send, ring_recv, pair_send, pair_recv, done_sem):
    me = lax.axis_index("dp")
    chips = devices // CORES
    z, core = lax.div(me, CORES), lax.rem(me, CORES)
    peer = me + 1 - 2 * core
    onward = (lax.rem(me + CORES, devices), lax.rem(me + devices - CORES, devices))
    _, matrices, depth, d_out = a_ref.shape
    ff = g_ref.shape[3]
    half, mine = d_out // 2, d_out // 4
    per_matrix = chips // matrices
    tiles = ff // per_matrix // NB
    steps = chips * tiles
    KB = min(2048, depth)
    early = tiles // 2
    late = tiles - early
    turn = chips * early

    def chunk(d, s):
        c = lax.rem(z + jnp.where(d == 0, chips - 1 - s, 1 + s), chips)
        return lax.div(c, per_matrix), lax.rem(c, per_matrix)

    def place(d, s, t):
        n, side = chunk(d, s)
        return n, pl.ds(pl.multiple_of((side * tiles + t) * NB, NB), NB)

    own = [pl.ds(pl.multiple_of(d * half + core * mine, 16), mine) for d in range(2)]
    theirs = [pl.ds(pl.multiple_of(d * half + (1 - core) * mine, 16), mine) for d in range(2)]
    own_acc = pl.ds(pl.multiple_of(core * mine, 16), mine)
    their_acc = pl.ds(pl.multiple_of((1 - core) * mine, 16), mine)

    def split(k):
        first = k < turn
        width = jnp.where(first, early, late)
        r = jnp.where(first, k, k - turn)
        return lax.div(r, width), lax.rem(r, width) + jnp.where(first, 0, early)

    def g_load(k, d):
        s, t = split(k)
        n, cols = place(d, s, t)
        slot = d + 2 * lax.rem(k, 2)
        return pltpu.make_async_copy(g_ref.at[0, n, :, cols], gbuf.at[slot], gsem.at[slot])

    def a_load(d, s):
        n, _ = chunk(d, s)
        lo = pl.multiple_of(d * (d_out - ROWS), AB)
        return pltpu.make_async_copy(a_ref.at[0, n, :, pl.ds(lo, ROWS)], abuf, asem)

    def fresh(s):
        return lax.rem(z + s, per_matrix)

    def transpose(d, s):
        n, _ = chunk(d, s)
        lo = d * (d_out - ROWS)

        def block(i, _):
            k, j = lax.div(i, ROWS // AB), lax.rem(i, ROWS // AB)
            ks = pl.ds(pl.multiple_of(k * KB, KB), KB)
            x = abuf[ks, pl.ds(pl.multiple_of(j * AB, AB), AB)]
            at[n, pl.ds(pl.multiple_of(lo + j * AB, AB), AB), ks] = x.T
            return 0

        lax.fori_loop(0, depth // KB * (ROWS // AB), block, 0)

    def ring_sum(d, s, n, cols, t):
        return pltpu.make_async_remote_copy(
            src_ref=sums.at[d, t], dst_ref=out_ref.at[n, own[d], cols], send_sem=sums_sem.at[d, t],
            recv_sem=ring_recv.at[d, s + 1, t], device_id={"dp": onward[d]}, device_id_type=MESH)

    def ring(d, src_idx, n, cols, dst_idx, t):
        piece = out_ref.at[n, own[d], cols]
        return pltpu.make_async_remote_copy(
            src_ref=piece, dst_ref=piece, send_sem=ring_send.at[d, src_idx, t], recv_sem=ring_recv.at[d, dst_idx, t],
            device_id={"dp": onward[d]}, device_id_type=MESH)

    def pair_out(d, k):
        s, t = split(k)
        n, cols = place(d, s, t)
        slot = lax.rem(k, 2)
        return pltpu.make_async_remote_copy(
            src_ref=stage.at[d, slot], dst_ref=out_ref.at[n, own[d], cols], send_sem=stage_sem.at[d, slot],
            recv_sem=pair_recv.at[d, s, t], device_id={"dp": peer}, device_id_type=MESH)

    def pair_share(d, j, n, cols, t):
        piece = out_ref.at[n, own[d], cols]
        return pltpu.make_async_remote_copy(
            src_ref=piece, dst_ref=piece, send_sem=pair_send.at[d, j, t], recv_sem=pair_recv.at[d, j, t],
            device_id={"dp": peer}, device_id_type=MESH)

    def products(k):
        s, _ = split(k)

        @pl.when(k + 1 < steps)
        def _():
            for d in range(2):
                g_load(k + 1, d).start()

        for d in range(2):
            g_load(k, d).wait()
        slot = lax.rem(k, 2)
        for d in range(2):
            n, _ = chunk(d, s)
            acc[slot, d] = jnp.dot(
                at[n, pl.ds(d * half, half), :], gbuf[d + 2 * slot], preferred_element_type=jnp.float32)

    def pair_up(k):
        slot = lax.rem(k, 2)

        @pl.when(k >= 2)
        def _():
            for d in range(2):
                pair_out(d, k - 2).wait_send()

        for d in range(2):
            stage[d, slot] = acc[slot, d, their_acc, :].astype(stage.dtype)
        for d in range(2):
            pair_out(d, k).start()

    def add(k, d):
        s, t = split(k)
        n, cols = place(d, s, t)

        @pl.when(s > 0)
        def _():
            ring_sum(d, s - 1, n, cols, t).wait()

        pair_share(d, s, n, cols, t).wait_recv()
        total = acc[lax.rem(k, 2), d, own_acc, :] + out_ref[n, theirs[d], cols].astype(jnp.float32)
        before = out_ref[n, own[d], cols].astype(jnp.float32)
        total = jnp.where(s > 0, total + before, total).astype(out_ref.dtype)

        @pl.when(s < chips - 1)
        def _():
            sums[d, t] = total
            ring_sum(d, s, n, cols, t).start()

        @pl.when(s == chips - 1)
        def _():
            out_ref[n, own[d], cols] = total
            ring(d, s, n, cols, 0, t).start()

    def greet():
        pl.semaphore_signal(done_sem, inc=1, device_id={"dp": peer}, device_id_type=MESH)

    def share_own(lo, hi):
        pl.semaphore_wait(done_sem, 1)

        def one(t, _):
            for d in range(2):
                n, cols = place(d, chips - 1, t)
                pair_share(d, chips - 1, n, cols, t).start()
            return 0

        lax.fori_loop(lo, hi, one, 0)

    def gather(j, t):
        for d in range(2):
            n, cols = place(d, j, t)
            ring(d, j, n, cols, j, t).wait_recv()

            @pl.when(j < chips - 2)
            def _():
                ring(d, j, n, cols, j + 1, t).start()

            pair_share(d, j, n, cols, t).start()

    barrier = pltpu.get_barrier_semaphore()
    for other in (*onward, peer):
        pl.semaphore_signal(barrier, inc=1, device_id={"dp": other}, device_id_type=MESH)
    for d in range(2):
        a_load(d, 0).start()
        if d == 0:
            for e in range(2):
                g_load(0, e).start()
        a_load(d, 0).wait()
        transpose(d, 0)
    a_load(fresh(1), 1).start()
    pl.semaphore_wait(barrier, 3)

    def reduce_early(k, _):
        s, t = split(k)
        products(k)
        pair_up(k)

        @pl.when(k > 0)
        def _():
            for d in range(2):
                add(k - 1, d)

        @pl.when(jnp.logical_and(t == 0, s + 1 < chips - 1))
        def _():
            a_load(fresh(s + 1), s + 1).wait()
            transpose(fresh(s + 1), s + 1)

            @pl.when(s + 2 < chips - 1)
            def _():
                a_load(fresh(s + 2), s + 2).start()

        return 0

    lax.fori_loop(0, turn, reduce_early, 0)

    hops, span = (chips - 1) * early, chips * late - 2

    def reduce_late(i, _):
        k = turn + i
        products(k)
        pair_up(k)
        for d in range(2):
            add(k - 1, d)

        @pl.when(i == 0)
        def _():
            greet()

        @pl.when(i == 1)
        def _():
            share_own(0, early)

        q = lax.div((i - 2) * hops, span)

        @pl.when(jnp.logical_and(i >= 2, lax.div((i - 1) * hops, span) > q))
        def _():
            gather(lax.div(q, early), lax.rem(q, early))

        return 0

    lax.fori_loop(0, chips * late, reduce_late, 0)
    for d in range(2):
        add(steps - 1, d)
    greet()
    share_own(early, tiles)

    def gather_late(i, _):
        gather(lax.div(i, late), early + lax.rem(i, late))
        return 0

    lax.fori_loop(0, (chips - 1) * late, gather_late, 0)

    def drain(i, _):
        j, t = lax.div(i, tiles), lax.rem(i, tiles)
        for d in range(2):
            n, cols = place(d, j, t)
            last = pair_share(d, j, n, cols, t)
            last.wait_send()
            last.wait_recv()

            @pl.when(j != chips - 2)
            def _():
                ring(d, j, n, cols, 0, t).wait_send()
        return 0

    lax.fori_loop(0, steps, drain, 0)
    for d in range(2):
        for k in (steps - 2, steps - 1):
            pair_out(d, k).wait_send()


def solution(mesh):
    devices = mesh.shape["dp"]

    def step(a, g):
        _, matrices, depth, d_out = a.shape
        ff = g.shape[3]
        chips = devices // CORES
        tiles = ff // (chips // matrices) // NB
        per = (2, chips, tiles)
        return pl.pallas_call(
            functools.partial(kernel, devices),
            out_shape=pltpu.VMEM((matrices, d_out, ff), a.dtype),
            in_specs=[pl.BlockSpec(memory_space=pl.ANY)] * 2,
            out_specs=pl.BlockSpec(memory_space=pltpu.VMEM),
            scratch_shapes=[
                pltpu.VMEM((matrices, d_out, depth), a.dtype),
                pltpu.VMEM((GSLOTS, depth, NB), g.dtype),
                pltpu.VMEM((depth, ROWS), a.dtype),
                pltpu.VMEM((2, 2, d_out // 2, NB), jnp.float32),
                pltpu.VMEM((2, 2, d_out // 4, NB), a.dtype),
                pltpu.VMEM((2, tiles, d_out // 4, NB), a.dtype),
                pltpu.SemaphoreType.DMA((GSLOTS,)),
                pltpu.SemaphoreType.DMA,
                pltpu.SemaphoreType.DMA((2, 2)),
                pltpu.SemaphoreType.DMA((2, tiles)),
                pltpu.SemaphoreType.DMA(per),
                pltpu.SemaphoreType.DMA(per),
                pltpu.SemaphoreType.DMA(per),
                pltpu.SemaphoreType.DMA(per),
                pltpu.SemaphoreType.REGULAR,
            ],
            compiler_params=pltpu.CompilerParams(
                collective_id=0, has_side_effects=True, vmem_limit_bytes=45 * 2**20,
            ),
        )(a, g)

    return jax.shard_map(
        step,
        mesh=mesh,
        in_specs=(P(("rep", "dp")), P(("rep", "dp"))),
        out_specs=P("rep"),
        check_vma=False,
    )
```

```python
import functools

import jax
import jax.numpy as jnp
from jax import lax
from jax.experimental import pallas as pl
from jax.experimental.pallas import tpu as pltpu
from jax.sharding import PartitionSpec as P

MESH = pl.DeviceIdType.MESH
CORES = 2
NB = 256
AB = 128
GDEPTH = 3
PIECES = 4
ROWS = 512
SLOTS = 3
LAG = 1


def kernel(devices, a_ref, g_ref, out_ref, at, gbuf, abuf, acc, stage, sums, gsem, asem, stage_sem, sums_sem,
           ring_send, ring_recv, pair_send, pair_recv, done_sem):
    me = lax.axis_index("dp")
    chips = devices // CORES
    z, core = lax.div(me, CORES), lax.rem(me, CORES)
    peer = me + 1 - 2 * core
    ahead = lax.rem(me + jnp.where(core == 0, CORES, devices - CORES), devices)
    behind = lax.rem(me + jnp.where(core == 0, devices - CORES, CORES), devices)
    _, matrices, depth, d_out = a_ref.shape
    ff = g_ref.shape[3]
    half = d_out // 2
    per_matrix = chips // matrices
    tiles = ff // per_matrix // NB
    steps = chips * tiles
    KB = depth // PIECES

    def chunk(d, s):
        c = lax.rem(z + jnp.where(d == 0, chips - 1 - s, 1 + s), chips)
        return lax.div(c, per_matrix), lax.rem(c, per_matrix)

    def place(d, s, t):
        n, side = chunk(d, s)
        return n, pl.ds(pl.multiple_of((side * tiles + t) * NB, NB), NB)

    own = pl.ds(pl.multiple_of(core * half, 16), half)
    theirs = pl.ds(pl.multiple_of((1 - core) * half, 16), half)

    def split(k):
        return lax.div(k, tiles), lax.rem(k, tiles)

    def g_load(k, d):
        s, t = split(k)
        n, cols = place(d, s, t)
        slot = d + 2 * lax.rem(k, GDEPTH)
        return pltpu.make_async_copy(g_ref.at[0, n, :, cols], gbuf.at[slot], gsem.at[slot])

    def a_load(d, s, q):
        n, _ = chunk(d, s)
        lo = pl.multiple_of(d * (d_out - ROWS), AB)
        return pltpu.make_async_copy(
            a_ref.at[0, n, pl.ds(pl.multiple_of(q * KB, KB), KB), pl.ds(lo, ROWS)],
            abuf.at[lax.rem(q, 2)], asem.at[lax.rem(q, 2)])

    def fresh(s):
        return lax.rem(z + s, per_matrix)

    def transpose(d, s, q):
        n, _ = chunk(d, s)
        lo = d * (d_out - ROWS)

        at[n, pl.ds(pl.multiple_of(lo, AB), ROWS), pl.ds(pl.multiple_of(q * KB, KB), KB)] = abuf[lax.rem(q, 2)].T

    def ring_sum(s, n, cols, t):
        slot = lax.rem(s * tiles + t, SLOTS)
        return pltpu.make_async_remote_copy(
            src_ref=sums.at[slot], dst_ref=out_ref.at[n, own, cols], send_sem=sums_sem.at[slot],
            recv_sem=ring_recv.at[s + 1, t], device_id={"dp": ahead}, device_id_type=MESH)

    def ring(src_idx, n, cols, dst_idx, t):
        piece = out_ref.at[n, own, cols]
        return pltpu.make_async_remote_copy(
            src_ref=piece, dst_ref=piece, send_sem=ring_send.at[src_idx, t], recv_sem=ring_recv.at[dst_idx, t],
            device_id={"dp": ahead}, device_id_type=MESH)

    def pair_out(k):
        s, t = split(k)
        n, cols = place(1 - core, s, t)
        slot = lax.rem(k, 2)
        return pltpu.make_async_remote_copy(
            src_ref=stage.at[slot], dst_ref=out_ref.at[n, own, cols], send_sem=stage_sem.at[slot],
            recv_sem=pair_recv.at[s, t], device_id={"dp": peer}, device_id_type=MESH)

    def pair_share(j, n, cols, t):
        piece = out_ref.at[n, own, cols]
        return pltpu.make_async_remote_copy(
            src_ref=piece, dst_ref=piece, send_sem=pair_send.at[j, t], recv_sem=pair_recv.at[j, t],
            device_id={"dp": peer}, device_id_type=MESH)

    def fetch(k):
        @pl.when(k + GDEPTH - 1 < steps)
        def _():
            for d in range(2):
                g_load(k + GDEPTH - 1, d).start()

        for d in range(2):
            g_load(k, d).wait()

    def free_stage(k):
        @pl.when(k >= 2)
        def _():
            pair_out(k - 2).wait_send()

    def products(k, beside=lambda: None):
        s, _ = split(k)
        terms = []
        for d in range(2):
            n, _ = chunk(d, s)
            terms.append(jnp.dot(
                at[n, pl.ds(d * half, half), :], gbuf[d + 2 * lax.rem(k, GDEPTH)], preferred_element_type=jnp.float32))
        beside()
        acc[lax.rem(k, LAG + 1)] = jnp.where(core == 0, terms[0], terms[1])
        stage[lax.rem(k, 2)] = jnp.where(core == 0, terms[1], terms[0]).astype(stage.dtype)

    def await_terms(k):
        s, t = split(k)
        n, cols = place(core, s, t)

        @pl.when(s > 0)
        def _():
            ring_sum(s - 1, n, cols, t).wait_recv()

        pair_share(s, n, cols, t).wait_recv()

        @pl.when(jnp.logical_and(k >= SLOTS, k - SLOTS < steps - tiles))
        def _():
            s0, t0 = split(k - SLOTS)
            n0, cols0 = place(core, s0, t0)
            ring_sum(s0, n0, cols0, t0).wait_send()

    def add(k):
        s, t = split(k)
        n, cols = place(core, s, t)
        total = acc[lax.rem(k, LAG + 1)] + out_ref[n, theirs, cols].astype(jnp.float32)
        before = out_ref[n, own, cols].astype(jnp.float32)
        sums[lax.rem(k, SLOTS)] = jnp.where(s > 0, total + before, total).astype(sums.dtype)

    def send(k):
        s, t = split(k)
        n, cols = place(core, s, t)

        @pl.when(s < chips - 1)
        def _():
            ring_sum(s, n, cols, t).start()

        @pl.when(s == chips - 1)
        def _():
            out_ref[n, own, cols] = sums[lax.rem(k, SLOTS)]
            ring(s, n, cols, 0, t).start()

    barrier = pltpu.get_barrier_semaphore()
    for other in (ahead, behind, peer):
        pl.semaphore_signal(barrier, inc=1, device_id={"dp": other}, device_id_type=MESH)
    def first_load(d, e):
        n, _ = chunk(d, 0)
        return pltpu.make_async_copy(
            a_ref.at[0, n, :, pl.ds(d * (d_out - ROWS) + e * NB, NB)], gbuf.at[2 + 2 * d + e], gsem.at[2 + 2 * d + e])

    for d in range(2):
        for e in range(2):
            first_load(d, e).start()
    for d in range(2):
        g_load(0, d).start()
    for q in range(2):
        a_load(fresh(1), 1, q).start()
    for d in range(2):
        n, _ = chunk(d, 0)
        for e in range(2):
            first_load(d, e).wait()

            def turn(q, _):
                ks = pl.ds(pl.multiple_of(q * KB, KB), KB)
                at[n, pl.ds(d * (d_out - ROWS) + e * NB, NB), ks] = gbuf[2 + 2 * d + e, ks, :].T
                return 0

            lax.fori_loop(0, PIECES, turn, 0)
    for k in range(1, GDEPTH - 1):
        for d in range(2):
            g_load(k, d).start()
    pl.semaphore_wait(barrier, 3)

    def next_matrix(k):
        s, q = split(k)

        @pl.when(jnp.logical_and(q < PIECES, s + 1 < chips - 1))
        def _():
            a_load(fresh(s + 1), s + 1, q).wait()
            transpose(fresh(s + 1), s + 1, q)

            @pl.when(q < PIECES - 2)
            def _():
                a_load(fresh(s + 1), s + 1, q + 2).start()

            @pl.when(jnp.logical_and(q >= PIECES - 2, s + 2 < chips - 1))
            def _():
                a_load(fresh(s + 2), s + 2, q + 2 - PIECES).start()

    def reduce_step(k, _):
        fetch(k)
        free_stage(k)
        products(k)
        pair_out(k).start()

        @pl.when(k >= LAG)
        def _():
            await_terms(k - LAG)
            add(k - LAG)
            send(k - LAG)

        next_matrix(k)
        return 0

    lax.fori_loop(0, steps, reduce_step, 0)

    def last_steps(k, _):
        await_terms(k)
        add(k)
        send(k)
        return 0

    lax.fori_loop(steps - LAG, steps, last_steps, 0)

    pl.semaphore_signal(done_sem, inc=1, device_id={"dp": peer}, device_id_type=MESH)
    pl.semaphore_wait(done_sem, 1)

    def share_own(t, _):
        n, cols = place(core, chips - 1, t)
        pair_share(chips - 1, n, cols, t).start()
        return 0

    lax.fori_loop(0, tiles, share_own, 0)

    def gather(i, _):
        j, t = split(i)
        n, cols = place(core, j, t)
        ring(j, n, cols, j, t).wait_recv()

        @pl.when(j < chips - 2)
        def _():
            ring(j, n, cols, j + 1, t).start()

        pair_share(j, n, cols, t).start()
        return 0

    lax.fori_loop(0, (chips - 1) * tiles, gather, 0)

    def drain(i, _):
        j, t = split(i)
        n, cols = place(core, j, t)
        last = pair_share(j, n, cols, t)
        last.wait_send()
        last.wait_recv()

        @pl.when(j != chips - 2)
        def _():
            ring(j, n, cols, 0, t).wait_send()
        return 0

    lax.fori_loop(0, steps, drain, 0)
    for k in (steps - 2, steps - 1):
        pair_out(k).wait_send()


def solution(mesh):
    devices = mesh.shape["dp"]

    def step(a, g):
        _, matrices, depth, d_out = a.shape
        ff = g.shape[3]
        chips = devices // CORES
        tiles = ff // (chips // matrices) // NB
        per = (chips, tiles)
        return pl.pallas_call(
            functools.partial(kernel, devices),
            out_shape=pltpu.VMEM((matrices, d_out, ff), a.dtype),
            in_specs=[pl.BlockSpec(memory_space=pl.ANY)] * 2,
            out_specs=pl.BlockSpec(memory_space=pltpu.VMEM),
            scratch_shapes=[
                pltpu.VMEM((matrices, d_out, depth), a.dtype),
                pltpu.VMEM((2 * GDEPTH, depth, NB), g.dtype),
                pltpu.VMEM((2, depth // PIECES, ROWS), a.dtype),
                pltpu.VMEM((LAG + 1, d_out // 2, NB), jnp.float32),
                pltpu.VMEM((2, d_out // 2, NB), a.dtype),
                pltpu.VMEM((SLOTS, d_out // 2, NB), a.dtype),
                pltpu.SemaphoreType.DMA((2 * GDEPTH,)),
                pltpu.SemaphoreType.DMA((2,)),
                pltpu.SemaphoreType.DMA((2,)),
                pltpu.SemaphoreType.DMA((SLOTS,)),
                pltpu.SemaphoreType.DMA(per),
                pltpu.SemaphoreType.DMA(per),
                pltpu.SemaphoreType.DMA(per),
                pltpu.SemaphoreType.DMA(per),
                pltpu.SemaphoreType.REGULAR,
            ],
            compiler_params=pltpu.CompilerParams(
                collective_id=0, has_side_effects=True, vmem_limit_bytes=48_600_000,
            ),
        )(a, g)

    return jax.shard_map(
        step,
        mesh=mesh,
        in_specs=(P(("rep", "dp")), P(("rep", "dp"))),
        out_specs=P("rep"),
        check_vma=False,
    )
```
